32 devices in a mesh: row: 4 (over z), col: 8 (over y, x, core).
Axes of the slice: x: 2, y: 2, z: 4, core: 2. Of those that a mesh axis runs over, the one named last changes fastest.
Arguments:
- build_key: int32 [8, 8, 128], P('col', 'row'), may hold values from -1 to 63, as said below
- build_part: int32 [8, 8], P('col', 'row'), may hold values from 0 to 1023, as said below
- build_payload: float32 [8, 8, 128, 128], P('col', 'row'), may hold values from -6 to 6
- probe_key: int32 [4, 8, 8, 8, 128], P('row', 'col'), may hold values from -2 to 63, as said below
- probe_part: int32 [4, 8, 8, 8, 128], P('row', 'col'), may hold values from 0 to 1023, as said below
Outputs:
- joined: float32 [4, 8, 8, 8, 128, 128], P('row', 'col')
- match_position: float32 [4, 8, 8, 8, 128], P('row', 'col')
- match_rate: float32 [1024], replicated
The draws below stay inside these ranges and needn't reach their ends.
Inputs may be any that keep to these rules, and one draw needn't show every extreme that they name: Each column c owns a set of 128 partitions, disjoint from the other columns' sets; build_part[c, t] lies in column c's set. `build_key`: -1 marks padding rows, which lie at the end of a tile. `probe_key`: -2 marks padding rows, which lie at the end of a tile. probe_part[r, s, c, q, i] lies in the set of partitions owned by column c.
All inputs are finite; a program needn't handle non-finite values.
Results may differ from the reference program's by a relative error of at most 0.0003.
Values sent between devices are 32-bit elements; how exact they have to be, the bound alone decides.
A program may use at most 256 MiB of HBM per device.

```python
import jax
import jax.numpy as jnp
from jax import lax

PARTS_SIZE = 1024
TILE = 128
PAYLOAD = 128
KEY_RANGE = 64
PROBE_TILES = 8
COLUMN_TILES = 8
N_ROW = 4
N_COL = 8


def owned_table(key):
    shuffled = jax.random.permutation(jax.random.fold_in(key, 7), PARTS_SIZE)
    return shuffled.reshape(N_COL, PARTS_SIZE // N_COL).astype(jnp.int32)


def skewed_pick(key, dims):
    share = PARTS_SIZE // N_COL
    picked = jax.random.randint(key, dims, 0, share)
    return picked * picked // share


def draw_build_part(key, part):
    table = owned_table(key)
    picks = skewed_pick(jax.random.fold_in(key, 1), (N_COL, COLUMN_TILES))
    owners = jnp.arange(N_COL)[:, None]
    return table[owners, picks].astype(jnp.int32)


def draw_build_key(key, part):
    base = jax.random.randint(jax.random.fold_in(key, 2), (N_COL, COLUMN_TILES, TILE), 0, KEY_RANGE)
    filled = jax.random.randint(jax.random.fold_in(key, 3), (N_COL, COLUMN_TILES, 1), TILE // 4, TILE + 1)
    places = jnp.arange(TILE)[None, None, :]
    return jnp.where(places < filled, base, -1).astype(jnp.int32)


def draw_probe_part(key, part):
    table = owned_table(key)
    picks = skewed_pick(jax.random.fold_in(key, 4), (N_ROW, N_COL, N_COL, PROBE_TILES, TILE))
    owners = jnp.arange(N_COL)[None, None, :, None, None]
    return table[owners, picks].astype(jnp.int32)


def draw_probe_key(key, part):
    base = jax.random.randint(jax.random.fold_in(key, 5), (N_ROW, N_COL, N_COL, PROBE_TILES, TILE), 0, KEY_RANGE)
    filled = jax.random.randint(jax.random.fold_in(key, 6), (N_ROW, N_COL, N_COL, PROBE_TILES, 1), TILE // 4, TILE + 1)
    places = jnp.arange(TILE)[None, None, None, None, :]
    return jnp.where(places < filled, base, -2).astype(jnp.int32)


def shard_levels(stream_key, shape, split, low, largest):
    level, own = 1.0, jax.random.fold_in(stream_key, 6)
    for axis_at, blocks in split:
        draws = jnp.exp(jax.random.uniform(jax.random.fold_in(own, axis_at), (blocks,), jnp.float32, low / len(split), largest / len(split)))
        level = level * jnp.repeat(draws, shape[axis_at] // blocks).reshape([-1 if axis == axis_at else 1 for axis in range(len(shape))])
    return level


def centred(stream_key, shape, width, bound, cuts=(), held_as=jnp.bfloat16):
    values = width * jax.random.normal(stream_key, shape, jnp.float32)
    if cuts:
        values = values * shard_levels(stream_key, shape, cuts, -0.22, 0.18)
    return jnp.clip(values, -bound, bound).astype(held_as)


def setup_inputs(seed: int = 0) -> dict:
    arg_keys = jax.random.split(jax.random.key(seed), 6)
    build_key = draw_build_key(jax.random.fold_in(arg_keys[5], 71), 0)
    build_part = draw_build_part(jax.random.fold_in(arg_keys[5], 71), 0)
    build_payload = centred(arg_keys[2], (N_COL, COLUMN_TILES, TILE, PAYLOAD), 1.0, 6.0, ((0, 8), (1, 4)), jnp.float32)
    probe_key = draw_probe_key(jax.random.fold_in(arg_keys[5], 71), 0)
    probe_part = draw_probe_part(jax.random.fold_in(arg_keys[5], 71), 0)
    return dict(build_key=build_key, build_part=build_part, build_payload=build_payload, probe_key=probe_key, probe_part=probe_part)


def tile_join(probe_keys, probe_parts, build_keys, build_parts, payload, positions):
    count_tiles = build_keys.shape[0]
    tile_rows = build_keys.shape[1]
    flat_keys = build_keys.reshape(-1)
    flat_parts = jnp.broadcast_to(build_parts.reshape(-1, 1), (count_tiles, tile_rows)).reshape(-1)
    flat_payload = payload.reshape(count_tiles * tile_rows, payload.shape[-1])

    def one_block(block_args):
        block_keys, block_parts = block_args
        matched = ((block_keys[:, None] == flat_keys[None, :]) & (block_parts[:, None] == flat_parts[None, :])).astype(jnp.float32)
        summed = jnp.dot(matched, flat_payload, precision=lax.Precision.HIGHEST, preferred_element_type=jnp.float32)
        placed = jnp.dot(matched, positions, precision=lax.Precision.HIGHEST, preferred_element_type=jnp.float32)
        return summed, placed, jnp.sum(matched, axis=1)

    return lax.map(one_block, (probe_keys, probe_parts))


def reference(build_key, build_part, build_payload, probe_key, probe_part):
    positions = jnp.arange(COLUMN_TILES * TILE, dtype=jnp.int32).astype(jnp.float32) / float(COLUMN_TILES * TILE)

    def owner_block(index):
        row_index = index // N_COL
        col_index = index % N_COL
        keys_here = lax.dynamic_index_in_dim(probe_key, row_index, 0, keepdims=False)
        keys_here = lax.dynamic_index_in_dim(keys_here, col_index, 1, keepdims=False)
        parts_here = lax.dynamic_index_in_dim(probe_part, row_index, 0, keepdims=False)
        parts_here = lax.dynamic_index_in_dim(parts_here, col_index, 1, keepdims=False)
        build_keys = lax.dynamic_index_in_dim(build_key, col_index, 0, keepdims=False)
        build_parts = lax.dynamic_index_in_dim(build_part, col_index, 0, keepdims=False)
        payload = lax.dynamic_index_in_dim(build_payload, col_index, 0, keepdims=False)
        return tile_join(keys_here.reshape(N_COL, PROBE_TILES * TILE), parts_here.reshape(N_COL, PROBE_TILES * TILE), build_keys, build_parts, payload, positions)

    joined, placed, counts = lax.map(owner_block, jnp.arange(N_ROW * N_COL, dtype=jnp.int32))
    joined = joined.reshape(N_ROW, N_COL, N_COL, PROBE_TILES, TILE, PAYLOAD).transpose(0, 2, 1, 3, 4, 5)
    placed = placed.reshape(N_ROW, N_COL, N_COL, PROBE_TILES, TILE).transpose(0, 2, 1, 3, 4)
    counts = counts.reshape(N_ROW, N_COL, N_COL, PROBE_TILES, TILE).transpose(0, 2, 1, 3, 4)
    part_ids = probe_part.reshape(-1)
    match_total = jax.ops.segment_sum(counts.reshape(-1), part_ids, num_segments=PARTS_SIZE)
    live_rows = (probe_key >= 0).astype(jnp.float32).reshape(-1)
    live_total = jax.ops.segment_sum(live_rows, part_ids, num_segments=PARTS_SIZE)
    return joined, placed, match_total / jnp.maximum(live_total, 1.0)
```

```python
import functools

import jax
import jax.numpy as jnp
from jax import lax
from jax.experimental import pallas as pl
from jax.experimental.pallas import tpu as pltpu
from jax.sharding import PartitionSpec as P

PARTS_SIZE = 1024
KEY_RANGE = 64
LANES = 128
MESH = pl.DeviceIdType.MESH


def dot_nt(a, b):
    return lax.dot_general(a, b, (((1,), (1,)), ((), ())), preferred_element_type=jnp.float32)


def gather_kernel(
    rows, cols, local_tiles,
    bkey_ref, bpart_ref, pay_ref, pkey_ref, ppart_ref,
    tables_ref, smalls_ref, place_ref, rate_ref,
    own, hist1, hist2,
    small_send, small_recv, table_send, table_recv, pass_send, pass_recv,
    h1_send, h1_recv, h2_send, h2_recv, local_sem,
):
    r, c = lax.axis_index("row"), lax.axis_index("col")
    n = rows * cols
    chips = cols // 2
    me = r * cols + c
    partner = c + 1 - 2 * lax.rem(c, 2)
    parity = lax.rem(c, 2)

    def peer(k):
        pr = lax.rem(r + k // cols, rows)
        pc = lax.rem(c + lax.rem(k, cols), cols)
        return pr, pc

    barrier = pltpu.get_barrier_semaphore()

    @pl.loop(1, n)
    def _(k):
        pl.semaphore_signal(barrier, inc=1, device_id=peer(k), device_id_type=MESH)

    tile_rows = bkey_ref.shape[-1]
    depth = local_tiles * KEY_RANGE
    table = jnp.zeros((depth, pay_ref.shape[-1]), jnp.float32)
    small = jnp.zeros((8, depth), jnp.float32)
    sub = lax.broadcasted_iota(jnp.int32, (depth, tile_rows), 0)
    srow = lax.broadcasted_iota(jnp.int32, (8, tile_rows), 0)
    slane = lax.broadcasted_iota(jnp.int32, (8, tile_rows), 1)
    lane = lax.broadcasted_iota(jnp.int32, (8, depth), 1)
    orow = lax.broadcasted_iota(jnp.int32, (8, depth), 0)
    weights = jnp.where(srow == 0, 1, jnp.where(srow == 1, slane, 0)).astype(jnp.float32)
    part_lane = jnp.zeros((8, depth), jnp.int32)
    first_lane = jnp.zeros((8, depth), jnp.int32)
    for t in range(local_tiles):
        keys = bkey_ref[0, t : t + 1, :]
        hot = (sub - t * KEY_RANGE == keys) & (keys >= 0)
        hot = jnp.where(hot, 1.0, 0.0)
        table += jnp.dot(hot, pay_ref[0, t], precision=lax.Precision.HIGHEST, preferred_element_type=jnp.float32)
        small += dot_nt(weights, hot)
        mine = lane // KEY_RANGE == t
        part_lane = jnp.where(mine, bpart_ref[0, t], part_lane)
        first_lane = jnp.where(mine, (r * local_tiles + t) * tile_rows, first_lane)
    own[...] = table
    count = small[0:1, :]
    place = (small[1:2, :] + count * first_lane[0:1, :].astype(jnp.float32)) / float(rows * local_tiles * tile_rows)
    code = part_lane * KEY_RANGE + lax.rem(lane, KEY_RANGE)
    smalls_ref[me] = jnp.where(
        orow == 0, count, jnp.where(orow == 1, place, jnp.where(orow == 2, code.astype(jnp.float32), 0.0))
    )
    keep = pltpu.make_async_copy(own, tables_ref.at[me], local_sem)
    keep.start()

    pl.semaphore_wait(barrier, n - 1)

    def small_copy(k):
        return pltpu.make_async_remote_copy(
            src_ref=smalls_ref.at[me], dst_ref=smalls_ref.at[me], send_sem=small_send, recv_sem=small_recv,
            device_id=peer(k), device_id_type=MESH)

    @pl.loop(1, n)
    def _(k):
        small_copy(k).start()

    def chip_peer(k):
        return lax.rem(r + k // chips, rows), lax.rem(c + 2 * lax.rem(k, chips), cols)

    def chip_source(k):
        return lax.rem(r + rows - k // chips, rows), lax.rem(c + cols - 2 * lax.rem(k, chips), cols)

    def table_copy(k):
        return pltpu.make_async_remote_copy(
            src_ref=own, dst_ref=tables_ref.at[me], send_sem=table_send, recv_sem=table_recv.at[k],
            device_id=chip_peer(k), device_id_type=MESH)

    @pl.loop(1, rows * chips)
    def _(k):
        table_copy(k).start()

    def pass_copy(slot, src):
        return pltpu.make_async_remote_copy(
            src_ref=src, dst_ref=tables_ref.at[slot], send_sem=pass_send, recv_sem=pass_recv,
            device_id=(r, partner), device_id_type=MESH)

    pass_copy(me, own).start()

    smalls_rest = smalls_ref.at[pl.ds(0, n - 1)]
    pltpu.make_async_copy(smalls_rest, smalls_rest, small_recv).wait()
    probe_tiles = pkey_ref.shape[3]
    hi_iota = lax.broadcasted_iota(jnp.int32, (PARTS_SIZE // LANES, LANES), 0)
    lo_iota = lax.broadcasted_iota(jnp.int32, (LANES, LANES), 0)
    groups = PARTS_SIZE // LANES

    def owner_step(o, acc):
        keys = pkey_ref[0, 0, o]
        parts = ppart_ref[0, 0, o]
        live = keys >= 0
        code = (parts * KEY_RANGE + keys).astype(jnp.float32)
        counts = jnp.zeros(keys.shape, jnp.float32)
        places = jnp.zeros(keys.shape, jnp.float32)
        for sr in range(rows):
            block = smalls_ref[sr * cols + o]
            tabs = [jnp.broadcast_to(block[j : j + 1, :], (probe_tiles, depth)) for j in range(3)]
            for t in range(local_tiles):
                index = jnp.where(live, keys, 0) + t * KEY_RANGE
                got = [jnp.take_along_axis(tab, index, axis=1) for tab in tabs]
                hit = live & (got[2] == code)
                counts += jnp.where(hit, got[0], 0.0)
                places += jnp.where(hit, got[1], 0.0)
        place_ref[o] = places
        big = jnp.floor(counts * (1.0 / 256.0))
        rest = counts - 256.0 * big
        alive = jnp.where(live, 1.0, 0.0)
        hi = parts // LANES
        lo = lax.rem(parts, LANES)
        for q in range(probe_tiles):
            hot_hi = hi_iota == hi[q : q + 1, :]
            lhs = jnp.concatenate(
                [jnp.where(hot_hi, v[q : q + 1, :], 0.0) for v in (rest, big, alive)]
                + [jnp.zeros((groups, LANES), jnp.float32)], axis=0)
            rhs = jnp.where(lo_iota == lo[q : q + 1, :], 1.0, 0.0)
            acc += dot_nt(lhs.astype(jnp.bfloat16), rhs.astype(jnp.bfloat16))
        return acc

    acc = lax.fori_loop(0, cols, owner_step, jnp.zeros((4 * groups, LANES), jnp.float32))
    hist1[c, 0:groups, :] = acc[0:groups] + 256.0 * acc[groups : 2 * groups]
    hist1[c, groups : 2 * groups, :] = acc[2 * groups : 3 * groups]

    def h1_copy(k):
        return pltpu.make_async_remote_copy(
            src_ref=hist1.at[c], dst_ref=hist1.at[c], send_sem=h1_send, recv_sem=h1_recv,
            device_id=(r, lax.rem(c + k, cols)), device_id_type=MESH)

    @pl.loop(1, cols)
    def _(k):
        h1_copy(k).start()

    @pl.loop(1, rows * chips)
    def _(k):
        sr, sc = chip_source(k)
        slot = sr * cols + sc
        pltpu.make_async_copy(tables_ref.at[slot], tables_ref.at[slot], table_recv.at[k]).wait()
        pass_copy(slot, tables_ref.at[slot]).start()

    hist1_rest = hist1.at[pl.ds(0, cols - 1)]
    pltpu.make_async_copy(hist1_rest, hist1_rest, h1_recv).wait()
    hist2[r] = functools.reduce(lambda a, b: a + b, [hist1[j] for j in range(cols)])

    @pl.loop(1, rows)
    def _(k):
        pltpu.make_async_remote_copy(
            src_ref=hist2.at[r], dst_ref=hist2.at[r], send_sem=h2_send, recv_sem=h2_recv,
            device_id=(lax.rem(r + k, rows), c), device_id_type=MESH).start()

    hist2_rest = hist2.at[pl.ds(0, rows - 1)]
    pltpu.make_async_copy(hist2_rest, hist2_rest, h2_recv).wait()
    total = functools.reduce(lambda a, b: a + b, [hist2[j] for j in range(rows)])
    rate_ref[...] = total[0:groups] / jnp.maximum(total[groups : 2 * groups], 1.0)

    keep.wait()
    pltpu.make_async_copy(smalls_rest, smalls_rest, small_send).wait()
    pltpu.make_async_copy(hist1_rest, hist1_rest, h1_send).wait()
    pltpu.make_async_copy(hist2_rest, hist2_rest, h2_send).wait()
    others = tables_ref.at[pl.ds(0, rows * chips - 1)]
    pltpu.make_async_copy(others, others, table_send).wait()
    passed = tables_ref.at[pl.ds(0, rows * chips)]
    pltpu.make_async_copy(passed, passed, pass_send).wait()
    pltpu.make_async_copy(passed, passed, pass_recv).wait()


def join_kernel(tables_ref, smalls_ref, pkey_ref, ppart_ref, place_ref, rate_ref, joined_ref, place_out, rate_out):
    rows, _, depth, width = tables_ref.shape
    probe_tiles, tile_rows = pkey_ref.shape[3], pkey_ref.shape[4]
    table = tables_ref[...].reshape(rows * depth, width)
    high = table.astype(jnp.bfloat16)
    low = (table - high.astype(jnp.float32)).astype(jnp.bfloat16)
    both = jnp.concatenate([high, low], axis=1)
    keys = pkey_ref[0, 0, 0]
    code = jnp.where(keys >= 0, ppart_ref[0, 0, 0] * KEY_RANGE + keys, -1).astype(jnp.float32)
    code = code.T
    for q in range(probe_tiles):
        wide = jnp.broadcast_to(code[:, q : q + 1], (tile_rows, depth))
        hot = jnp.concatenate(
            [jnp.where(wide == smalls_ref[s, 0, 2:3, :], 1.0, 0.0).astype(jnp.bfloat16) for s in range(rows)], axis=1)
        out = jnp.dot(hot, both, preferred_element_type=jnp.float32)
        joined_ref[0, 0, 0, q] = out[:, :width] + out[:, width:]
    place_out[...] = place_ref[...].reshape(place_out.shape)
    rate_out[...] = rate_ref[...]


def local(build_key, build_part, build_payload, probe_key, probe_part):
    rows, cols = lax.axis_size("row"), lax.axis_size("col")
    n = rows * cols
    local_tiles = build_key.shape[1]
    width = build_payload.shape[-1]
    owners, probe_tiles, tile_rows = probe_key.shape[2:]
    depth = local_tiles * KEY_RANGE
    groups = PARTS_SIZE // LANES
    vmem = pl.BlockSpec(memory_space=pltpu.VMEM)
    dma = pltpu.SemaphoreType.DMA
    f32 = jnp.float32
    tables, smalls, places, rate = pl.pallas_call(
        functools.partial(gather_kernel, rows, cols, local_tiles),
        out_shape=(
            jax.ShapeDtypeStruct((n, depth, width), f32),
            jax.ShapeDtypeStruct((n, 8, depth), f32),
            jax.ShapeDtypeStruct((owners, probe_tiles, tile_rows), f32),
            jax.ShapeDtypeStruct((groups, LANES), f32),
        ),
        in_specs=[vmem, pl.BlockSpec(memory_space=pltpu.SMEM), vmem, vmem, vmem],
        out_specs=(vmem, vmem, vmem, vmem),
        scratch_shapes=[
            pltpu.VMEM((depth, width), f32),
            pltpu.VMEM((cols, 2 * groups, LANES), f32),
            pltpu.VMEM((rows, 2 * groups, LANES), f32),
            dma, dma, dma, dma((rows * (cols // 2),)), dma, dma,
            dma, dma, dma, dma, dma,
        ],
        compiler_params=pltpu.CompilerParams(
            collective_id=0, has_side_effects=True, vmem_limit_bytes=40 * 1024 * 1024
        ),
    )(build_key, build_part, build_payload, probe_key, probe_part)
    tables = tables.reshape(rows, cols, depth, width)
    smalls = smalls.reshape(rows, cols, 8, depth)
    joined, placed, rate = pl.pallas_call(
        join_kernel,
        grid=(owners,),
        out_shape=(
            jax.ShapeDtypeStruct((1, 1, owners, probe_tiles, tile_rows, width), f32),
            jax.ShapeDtypeStruct((1, 1, owners, probe_tiles, tile_rows), f32),
            jax.ShapeDtypeStruct((groups, LANES), f32),
        ),
        in_specs=[
            pl.BlockSpec((rows, 1, depth, width), lambda i: (0, i, 0, 0)),
            pl.BlockSpec((rows, 1, 8, depth), lambda i: (0, i, 0, 0)),
            pl.BlockSpec((1, 1, 1, probe_tiles, tile_rows), lambda i: (0, 0, i, 0, 0)),
            pl.BlockSpec((1, 1, 1, probe_tiles, tile_rows), lambda i: (0, 0, i, 0, 0)),
            pl.BlockSpec((1, probe_tiles, tile_rows), lambda i: (i, 0, 0)),
            pl.BlockSpec((groups, LANES), lambda i: (0, 0)),
        ],
        out_specs=(
            pl.BlockSpec((1, 1, 1, probe_tiles, tile_rows, width), lambda i: (0, 0, i, 0, 0, 0)),
            pl.BlockSpec((1, 1, 1, probe_tiles, tile_rows), lambda i: (0, 0, i, 0, 0)),
            pl.BlockSpec((groups, LANES), lambda i: (0, 0)),
        ),
    )(tables, smalls, probe_key, probe_part, places, rate)
    return joined, placed, rate.reshape(PARTS_SIZE)


def solution(mesh):
    return jax.shard_map(
        local,
        mesh=mesh,
        in_specs=(
            P("col", "row", None),
            P("col", "row"),
            P("col", "row", None, None),
            P("row", "col", None, None, None),
            P("row", "col", None, None, None),
        ),
        out_specs=(P("row", "col", None, None, None, None), P("row", "col", None, None, None), P()),
        check_vma=False,
    )
```

```python
import functools

import jax
import jax.numpy as jnp
from jax import lax
from jax.experimental import pallas as pl
from jax.experimental.pallas import tpu as pltpu
from jax.sharding import PartitionSpec as P

PARTS_SIZE = 1024
KEY_RANGE = 64
LANES = 128
MESH = pl.DeviceIdType.MESH


def dot_nt(a, b):
    return lax.dot_general(a, b, (((1,), (1,)), ((), ())), preferred_element_type=jnp.float32)


def gather_kernel(
    rows, cols, local_tiles,
    bkey_hbm, bpart_hbm, pay_hbm, pkey_hbm, ppart_hbm,
    tables_ref, smalls_ref, place_ref, rate_ref,
    bkey_ref, bpart_ref, pay_ref, pkey_ref, ppart_ref,
    own, hist1, hist2, in_sem,
    small_send, small_recv, table_send, table_recv, pass_send, pass_recv,
    h1_send, h1_recv, h2_send, h2_recv, local_sem,
):
    r, c = lax.axis_index("row"), lax.axis_index("col")
    n = rows * cols
    chips = cols // 2
    me = r * cols + c
    partner = c + 1 - 2 * lax.rem(c, 2)
    parity = lax.rem(c, 2)

    def peer(k):
        pr = lax.rem(r + k // cols, rows)
        pc = lax.rem(c + lax.rem(k, cols), cols)
        return pr, pc

    pairs = (
        (bkey_hbm, bkey_ref), (bpart_hbm, bpart_ref), (pay_hbm, pay_ref), (pkey_hbm, pkey_ref), (ppart_hbm, ppart_ref)
    )
    loads = [pltpu.make_async_copy(src, dst, in_sem.at[i]) for i, (src, dst) in enumerate(pairs)]
    for load in loads:
        load.start()
    barrier = pltpu.get_barrier_semaphore()

    @pl.loop(1, n)
    def _(k):
        pl.semaphore_signal(barrier, inc=1, device_id=peer(k), device_id_type=MESH)

    for load in loads[:3]:
        load.wait()
    tile_rows = bkey_ref.shape[-1]
    depth = local_tiles * KEY_RANGE
    table = jnp.zeros((depth, pay_ref.shape[-1]), jnp.float32)
    small = jnp.zeros((8, depth), jnp.float32)
    sub = lax.broadcasted_iota(jnp.int32, (depth, tile_rows), 0)
    srow = lax.broadcasted_iota(jnp.int32, (8, tile_rows), 0)
    slane = lax.broadcasted_iota(jnp.int32, (8, tile_rows), 1)
    lane = lax.broadcasted_iota(jnp.int32, (8, depth), 1)
    orow = lax.broadcasted_iota(jnp.int32, (8, depth), 0)
    weights = jnp.where(srow == 0, 1, jnp.where(srow == 1, slane, 0)).astype(jnp.float32)
    part_lane = jnp.zeros((8, depth), jnp.int32)
    first_lane = jnp.zeros((8, depth), jnp.int32)
    for t in range(local_tiles):
        keys = bkey_ref[0, t : t + 1, :]
        hot = (sub - t * KEY_RANGE == keys) & (keys >= 0)
        hot = jnp.where(hot, 1.0, 0.0)
        table += jnp.dot(hot, pay_ref[0, t], precision=lax.Precision.HIGHEST, preferred_element_type=jnp.float32)
        small += dot_nt(weights, hot)
        mine = lane // KEY_RANGE == t
        part_lane = jnp.where(mine, bpart_ref[0, t], part_lane)
        first_lane = jnp.where(mine, (r * local_tiles + t) * tile_rows, first_lane)
    own[...] = table
    count = small[0:1, :]
    place = (small[1:2, :] + count * first_lane[0:1, :].astype(jnp.float32)) / float(rows * local_tiles * tile_rows)
    code = part_lane * KEY_RANGE + lax.rem(lane, KEY_RANGE)
    smalls_ref[me] = jnp.where(
        orow == 0, count, jnp.where(orow == 1, place, jnp.where(orow == 2, code.astype(jnp.float32), 0.0))
    )
    keep = pltpu.make_async_copy(own, tables_ref.at[me], local_sem)
    keep.start()

    pl.semaphore_wait(barrier, n - 1)

    def small_copy(k):
        return pltpu.make_async_remote_copy(
            src_ref=smalls_ref.at[me], dst_ref=smalls_ref.at[me], send_sem=small_send, recv_sem=small_recv,
            device_id=peer(k), device_id_type=MESH)

    @pl.loop(1, n)
    def _(k):
        small_copy(k).start()

    def chip_peer(k):
        return lax.rem(r + k // chips, rows), lax.rem(c + 2 * lax.rem(k, chips), cols)

    def chip_source(k):
        return lax.rem(r + rows - k // chips, rows), lax.rem(c + cols - 2 * lax.rem(k, chips), cols)

    def table_copy(k):
        return pltpu.make_async_remote_copy(
            src_ref=own, dst_ref=tables_ref.at[me], send_sem=table_send, recv_sem=table_recv.at[k],
            device_id=chip_peer(k), device_id_type=MESH)

    @pl.loop(1, rows * chips)
    def _(k):
        table_copy(k).start()

    def pass_copy(slot, src):
        return pltpu.make_async_remote_copy(
            src_ref=src, dst_ref=tables_ref.at[slot], send_sem=pass_send, recv_sem=pass_recv,
            device_id=(r, partner), device_id_type=MESH)

    pass_copy(me, own).start()

    for load in loads[3:]:
        load.wait()
    smalls_rest = smalls_ref.at[pl.ds(0, n - 1)]
    pltpu.make_async_copy(smalls_rest, smalls_rest, small_recv).wait()
    probe_tiles = pkey_ref.shape[3]
    hi_iota = lax.broadcasted_iota(jnp.int32, (PARTS_SIZE // LANES, LANES), 0)
    lo_iota = lax.broadcasted_iota(jnp.int32, (LANES, LANES), 0)
    groups = PARTS_SIZE // LANES

    def owner_step(o, acc):
        keys = pkey_ref[0, 0, o]
        parts = ppart_ref[0, 0, o]
        live = keys >= 0
        code = (parts * KEY_RANGE + keys).astype(jnp.float32)
        counts = jnp.zeros(keys.shape, jnp.float32)
        places = jnp.zeros(keys.shape, jnp.float32)
        for sr in range(rows):
            block = smalls_ref[sr * cols + o]
            tabs = [jnp.broadcast_to(block[j : j + 1, :], (probe_tiles, depth)) for j in range(3)]
            for t in range(local_tiles):
                index = jnp.where(live, keys, 0) + t * KEY_RANGE
                got = [jnp.take_along_axis(tab, index, axis=1) for tab in tabs]
                hit = live & (got[2] == code)
                counts += jnp.where(hit, got[0], 0.0)
                places += jnp.where(hit, got[1], 0.0)
        place_ref[o] = places
        big = jnp.floor(counts * (1.0 / 256.0))
        rest = counts - 256.0 * big
        alive = jnp.where(live, 1.0, 0.0)
        hi = parts // LANES
        lo = lax.rem(parts, LANES)
        lhs, rhs = [], []
        for q in range(probe_tiles):
            hot_hi = hi_iota == hi[q : q + 1, :]
            lhs.append(jnp.concatenate(
                [jnp.where(hot_hi, v[q : q + 1, :], 0.0) for v in (rest, big, alive)]
                + [jnp.zeros((groups, LANES), jnp.float32)], axis=0).astype(jnp.bfloat16))
            rhs.append(jnp.where(lo_iota == lo[q : q + 1, :], 1.0, 0.0).astype(jnp.bfloat16))
        return acc + dot_nt(jnp.concatenate(lhs, axis=1), jnp.concatenate(rhs, axis=1))

    acc = lax.fori_loop(0, cols, owner_step, jnp.zeros((4 * groups, LANES), jnp.float32))
    hist1[c, 0:groups, :] = acc[0:groups] + 256.0 * acc[groups : 2 * groups]
    hist1[c, groups : 2 * groups, :] = acc[2 * groups : 3 * groups]

    def h1_copy(k):
        return pltpu.make_async_remote_copy(
            src_ref=hist1.at[c], dst_ref=hist1.at[c], send_sem=h1_send, recv_sem=h1_recv,
            device_id=(r, lax.rem(c + k, cols)), device_id_type=MESH)

    @pl.loop(1, cols)
    def _(k):
        h1_copy(k).start()

    @pl.loop(1, rows * chips)
    def _(k):
        sr, sc = chip_source(k)
        slot = sr * cols + sc
        pltpu.make_async_copy(tables_ref.at[slot], tables_ref.at[slot], table_recv.at[k]).wait()
        pass_copy(slot, tables_ref.at[slot]).start()

    hist1_rest = hist1.at[pl.ds(0, cols - 1)]
    pltpu.make_async_copy(hist1_rest, hist1_rest, h1_recv).wait()
    hist2[r] = functools.reduce(lambda a, b: a + b, [hist1[j] for j in range(cols)])

    @pl.loop(1, rows)
    def _(k):
        pltpu.make_async_remote_copy(
            src_ref=hist2.at[r], dst_ref=hist2.at[r], send_sem=h2_send, recv_sem=h2_recv,
            device_id=(lax.rem(r + k, rows), c), device_id_type=MESH).start()

    hist2_rest = hist2.at[pl.ds(0, rows - 1)]
    pltpu.make_async_copy(hist2_rest, hist2_rest, h2_recv).wait()
    total = functools.reduce(lambda a, b: a + b, [hist2[j] for j in range(rows)])
    rate_ref[...] = total[0:groups] / jnp.maximum(total[groups : 2 * groups], 1.0)

    keep.wait()
    pltpu.make_async_copy(smalls_rest, smalls_rest, small_send).wait()
    pltpu.make_async_copy(hist1_rest, hist1_rest, h1_send).wait()
    pltpu.make_async_copy(hist2_rest, hist2_rest, h2_send).wait()
    others = tables_ref.at[pl.ds(0, rows * chips - 1)]
    pltpu.make_async_copy(others, others, table_send).wait()
    passed = tables_ref.at[pl.ds(0, rows * chips)]
    pltpu.make_async_copy(passed, passed, pass_send).wait()
    pltpu.make_async_copy(passed, passed, pass_recv).wait()


def join_kernel(tables_ref, smalls_ref, pkey_ref, ppart_ref, place_ref, rate_ref, joined_ref, place_out, rate_out):
    owner = pl.program_id(0)
    rows, _, depth, width = tables_ref.shape
    probe_tiles, tile_rows = pkey_ref.shape[3], pkey_ref.shape[4]
    table = tables_ref[:, owner].reshape(rows * depth, width)
    high = table.astype(jnp.bfloat16)
    low = (table - high.astype(jnp.float32)).astype(jnp.bfloat16)
    both = jnp.concatenate([high, low], axis=1)
    keys = pkey_ref[0, 0, 0]
    code = jnp.where(keys >= 0, ppart_ref[0, 0, 0] * KEY_RANGE + keys, -1).astype(jnp.float32)
    code = code.T
    wanted = [smalls_ref[s, owner, 2:3, :] for s in range(rows)]
    hot = []
    for q in range(probe_tiles):
        wide = jnp.broadcast_to(code[:, q : q + 1], (tile_rows, depth))
        hot.append(jnp.concatenate(
            [jnp.where(wide == want, 1.0, 0.0).astype(jnp.bfloat16) for want in wanted], axis=1))
    out = jnp.dot(jnp.concatenate(hot, axis=0), both, preferred_element_type=jnp.float32)
    joined_ref[0, 0, 0] = (out[:, :width] + out[:, width:]).reshape(probe_tiles, tile_rows, width)
    place_out[...] = place_ref[owner].reshape(place_out.shape)
    rate_out[...] = rate_ref[...]


def local(build_key, build_part, build_payload, probe_key, probe_part):
    rows, cols = lax.axis_size("row"), lax.axis_size("col")
    n = rows * cols
    local_tiles = build_key.shape[1]
    width = build_payload.shape[-1]
    owners, probe_tiles, tile_rows = probe_key.shape[2:]
    depth = local_tiles * KEY_RANGE
    groups = PARTS_SIZE // LANES
    vmem = pl.BlockSpec(memory_space=pltpu.VMEM)
    dma = pltpu.SemaphoreType.DMA
    f32 = jnp.float32
    tables, smalls, places, rate = pl.pallas_call(
        functools.partial(gather_kernel, rows, cols, local_tiles),
        out_shape=(
            jax.ShapeDtypeStruct((n, depth, width), f32),
            jax.ShapeDtypeStruct((n, 8, depth), f32),
            jax.ShapeDtypeStruct((owners, probe_tiles, tile_rows), f32),
            jax.ShapeDtypeStruct((groups, LANES), f32),
        ),
        in_specs=[pl.BlockSpec(memory_space=pltpu.HBM)] * 5,
        out_specs=(vmem, vmem, vmem, vmem),
        scratch_shapes=[
            pltpu.VMEM(build_key.shape, build_key.dtype),
            pltpu.SMEM(build_part.shape, build_part.dtype),
            pltpu.VMEM(build_payload.shape, f32),
            pltpu.VMEM(probe_key.shape, probe_key.dtype),
            pltpu.VMEM(probe_part.shape, probe_part.dtype),
            pltpu.VMEM((depth, width), f32),
            pltpu.VMEM((cols, 2 * groups, LANES), f32),
            pltpu.VMEM((rows, 2 * groups, LANES), f32),
            dma((5,)),
            dma, dma, dma, dma((rows * (cols // 2),)), dma, dma,
            dma, dma, dma, dma, dma,
        ],
        compiler_params=pltpu.CompilerParams(
            collective_id=0, has_side_effects=True, vmem_limit_bytes=40 * 1024 * 1024
        ),
    )(build_key, build_part, build_payload, probe_key, probe_part)
    tables = tables.reshape(rows, cols, depth, width)
    smalls = smalls.reshape(rows, cols, 8, depth)
    joined, placed, rate = pl.pallas_call(
        join_kernel,
        grid=(owners,),
        out_shape=(
            jax.ShapeDtypeStruct((1, 1, owners, probe_tiles, tile_rows, width), f32),
            jax.ShapeDtypeStruct((1, 1, owners, probe_tiles, tile_rows), f32),
            jax.ShapeDtypeStruct((groups, LANES), f32),
        ),
        in_specs=[
            vmem,
            vmem,
            pl.BlockSpec((1, 1, 1, probe_tiles, tile_rows), lambda i: (0, 0, i, 0, 0)),
            pl.BlockSpec((1, 1, 1, probe_tiles, tile_rows), lambda i: (0, 0, i, 0, 0)),
            vmem,
            vmem,
        ],
        out_specs=(
            pl.BlockSpec((1, 1, 1, probe_tiles, tile_rows, width), lambda i: (0, 0, i, 0, 0, 0)),
            pl.BlockSpec((1, 1, 1, probe_tiles, tile_rows), lambda i: (0, 0, i, 0, 0)),
            pl.BlockSpec((groups, LANES), lambda i: (0, 0)),
        ),
        compiler_params=pltpu.CompilerParams(vmem_limit_bytes=24 * 1024 * 1024),
    )(tables, smalls, probe_key, probe_part, places, rate)
    return joined, placed, rate.reshape(PARTS_SIZE)


def solution(mesh):
    return jax.shard_map(
        local,
        mesh=mesh,
        in_specs=(
            P("col", "row", None),
            P("col", "row"),
            P("col", "row", None, None),
            P("row", "col", None, None, None),
            P("row", "col", None, None, None),
        ),
        out_specs=(P("row", "col", None, None, None, None), P("row", "col", None, None, None), P()),
        check_vma=False,
    )
```

```python
import functools

import jax
import jax.numpy as jnp
from jax import lax
from jax.experimental import pallas as pl
from jax.experimental.pallas import tpu as pltpu
from jax.sharding import PartitionSpec as P

PARTS_SIZE = 1024
KEY_RANGE = 64
LANES = 128
MESH = pl.DeviceIdType.MESH


def dot_nt(a, b):
    return lax.dot_general(a, b, (((1,), (1,)), ((), ())), preferred_element_type=jnp.float32)


def gather_kernel(
    rows, cols, local_tiles,
    bkey_hbm, bpart_hbm, pay_hbm, pkey_hbm, ppart_hbm,
    tables_ref, smalls_ref, place_ref, rate_ref,
    bkey_ref, bpart_ref, pay_ref, pkey_ref, ppart_ref,
    own, hist1, hist2, in_sem,
    small_send, small_recv, table_send, table_recv, pass_send, pass_recv,
    h1_send, h1_recv, h2_send, h2_recv, local_sem,
):
    r, c = lax.axis_index("row"), lax.axis_index("col")
    n = rows * cols
    chips = cols // 2
    me = r * cols + c
    partner = c + 1 - 2 * lax.rem(c, 2)
    parity = lax.rem(c, 2)

    def peer(k):
        pr = lax.rem(r + k // cols, rows)
        pc = lax.rem(c + lax.rem(k, cols), cols)
        return pr, pc

    pairs = (
        (bkey_hbm, bkey_ref), (bpart_hbm, bpart_ref), (pay_hbm, pay_ref), (pkey_hbm, pkey_ref), (ppart_hbm, ppart_ref)
    )
    loads = [pltpu.make_async_copy(src, dst, in_sem.at[i]) for i, (src, dst) in enumerate(pairs)]
    for load in loads:
        load.start()
    barrier = pltpu.get_barrier_semaphore()

    @pl.loop(1, n)
    def _(k):
        pl.semaphore_signal(barrier, inc=1, device_id=peer(k), device_id_type=MESH)

    for load in loads[:3]:
        load.wait()
    tile_rows = bkey_ref.shape[-1]
    depth = local_tiles * KEY_RANGE
    table = jnp.zeros((depth, pay_ref.shape[-1]), jnp.float32)
    small = jnp.zeros((8, depth), jnp.float32)
    sub = lax.broadcasted_iota(jnp.int32, (depth, tile_rows), 0)
    srow = lax.broadcasted_iota(jnp.int32, (8, tile_rows), 0)
    slane = lax.broadcasted_iota(jnp.int32, (8, tile_rows), 1)
    lane = lax.broadcasted_iota(jnp.int32, (8, depth), 1)
    orow = lax.broadcasted_iota(jnp.int32, (8, depth), 0)
    weights = jnp.where(srow == 0, 1, jnp.where(srow == 1, slane, 0)).astype(jnp.float32)
    part_lane = jnp.zeros((8, depth), jnp.int32)
    first_lane = jnp.zeros((8, depth), jnp.int32)
    for t in range(local_tiles):
        keys = bkey_ref[0, t : t + 1, :]
        hot = (sub - t * KEY_RANGE == keys) & (keys >= 0)
        hot = jnp.where(hot, 1.0, 0.0)
        table += jnp.dot(hot, pay_ref[0, t], precision=lax.Precision.HIGHEST, preferred_element_type=jnp.float32)
        small += dot_nt(weights, hot)
        mine = lane // KEY_RANGE == t
        part_lane = jnp.where(mine, bpart_ref[0, t], part_lane)
        first_lane = jnp.where(mine, (r * local_tiles + t) * tile_rows, first_lane)
    own[...] = table
    count = small[0:1, :]
    place = (small[1:2, :] + count * first_lane[0:1, :].astype(jnp.float32)) / float(rows * local_tiles * tile_rows)
    code = part_lane * KEY_RANGE + lax.rem(lane, KEY_RANGE)
    smalls_ref[me] = jnp.where(
        orow == 0, count, jnp.where(orow == 1, place, jnp.where(orow == 2, code.astype(jnp.float32), 0.0))
    )
    keep = pltpu.make_async_copy(own, tables_ref.at[me], local_sem)
    keep.start()

    pl.semaphore_wait(barrier, n - 1)

    def small_copy(k):
        return pltpu.make_async_remote_copy(
            src_ref=smalls_ref.at[me], dst_ref=smalls_ref.at[me], send_sem=small_send, recv_sem=small_recv,
            device_id=peer(k), device_id_type=MESH)

    @pl.loop(1, n)
    def _(k):
        small_copy(k).start()

    def chip_peer(k):
        return lax.rem(r + k // chips, rows), lax.rem(c + 2 * lax.rem(k, chips), cols)

    def chip_source(k):
        return lax.rem(r + rows - k // chips, rows), lax.rem(c + cols - 2 * lax.rem(k, chips), cols)

    def table_copy(k, src, slot, target):
        return pltpu.make_async_remote_copy(
            src_ref=src, dst_ref=tables_ref.at[slot], send_sem=table_send, recv_sem=table_recv.at[k],
            device_id=target, device_id_type=MESH)

    @pl.loop(1, rows)
    def _(i):
        table_copy(i * chips, own, me, chip_peer(i * chips)).start()

    @pl.loop(1, chips)
    def _(j):
        table_copy(j, own, me, chip_peer(j)).start()

    def pass_copy(slot, src):
        return pltpu.make_async_remote_copy(
            src_ref=src, dst_ref=tables_ref.at[slot], send_sem=pass_send, recv_sem=pass_recv,
            device_id=(r, partner), device_id_type=MESH)

    pass_copy(me, own).start()

    for load in loads[3:]:
        load.wait()
    smalls_rest = smalls_ref.at[pl.ds(0, n - 1)]
    pltpu.make_async_copy(smalls_rest, smalls_rest, small_recv).wait()

    @pl.loop(1, rows)
    def _(i):
        sr, sc = chip_source(i * chips)
        slot = sr * cols + sc
        pltpu.make_async_copy(tables_ref.at[slot], tables_ref.at[slot], table_recv.at[i * chips]).wait()

        @pl.loop(1, chips)
        def _(j):
            table_copy(i * chips + j, tables_ref.at[slot], slot, chip_peer(j)).start()

        pass_copy(slot, tables_ref.at[slot]).start()

    probe_tiles = pkey_ref.shape[3]
    hi_iota = lax.broadcasted_iota(jnp.int32, (PARTS_SIZE // LANES, LANES), 0)
    lo_iota = lax.broadcasted_iota(jnp.int32, (LANES, LANES), 0)
    groups = PARTS_SIZE // LANES

    def owner_step(o, acc):
        keys = pkey_ref[0, 0, o]
        parts = ppart_ref[0, 0, o]
        live = keys >= 0
        code = (parts * KEY_RANGE + keys).astype(jnp.float32)
        counts = jnp.zeros(keys.shape, jnp.float32)
        places = jnp.zeros(keys.shape, jnp.float32)
        for sr in range(rows):
            block = smalls_ref[sr * cols + o]
            tabs = [jnp.broadcast_to(block[j : j + 1, :], (probe_tiles, depth)) for j in range(3)]
            for t in range(local_tiles):
                index = jnp.where(live, keys, 0) + t * KEY_RANGE
                got = [jnp.take_along_axis(tab, index, axis=1) for tab in tabs]
                hit = live & (got[2] == code)
                counts += jnp.where(hit, got[0], 0.0)
                places += jnp.where(hit, got[1], 0.0)
        place_ref[o] = places
        big = jnp.floor(counts * (1.0 / 256.0))
        rest = counts - 256.0 * big
        alive = jnp.where(live, 1.0, 0.0)
        hi = parts // LANES
        lo = lax.rem(parts, LANES)
        lhs, rhs = [], []
        for q in range(probe_tiles):
            hot_hi = hi_iota == hi[q : q + 1, :]
            lhs.append(jnp.concatenate(
                [jnp.where(hot_hi, v[q : q + 1, :], 0.0) for v in (rest, big, alive)]
                + [jnp.zeros((groups, LANES), jnp.float32)], axis=0).astype(jnp.bfloat16))
            rhs.append(jnp.where(lo_iota == lo[q : q + 1, :], 1.0, 0.0).astype(jnp.bfloat16))
        return acc + dot_nt(jnp.concatenate(lhs, axis=1), jnp.concatenate(rhs, axis=1))

    acc = lax.fori_loop(0, cols, owner_step, jnp.zeros((4 * groups, LANES), jnp.float32))
    hist1[c, 0:groups, :] = acc[0:groups] + 256.0 * acc[groups : 2 * groups]
    hist1[c, groups : 2 * groups, :] = acc[2 * groups : 3 * groups]

    def h1_copy(k):
        return pltpu.make_async_remote_copy(
            src_ref=hist1.at[c], dst_ref=hist1.at[c], send_sem=h1_send, recv_sem=h1_recv,
            device_id=(r, lax.rem(c + k, cols)), device_id_type=MESH)

    @pl.loop(1, cols)
    def _(k):
        h1_copy(k).start()

    @pl.loop(0, rows * (chips - 1))
    def _(k):
        at = k // (chips - 1) * chips + lax.rem(k, chips - 1) + 1
        sr, sc = chip_source(at)
        slot = sr * cols + sc
        pltpu.make_async_copy(tables_ref.at[slot], tables_ref.at[slot], table_recv.at[at]).wait()
        pass_copy(slot, tables_ref.at[slot]).start()

    hist1_rest = hist1.at[pl.ds(0, cols - 1)]
    pltpu.make_async_copy(hist1_rest, hist1_rest, h1_recv).wait()
    hist2[r] = functools.reduce(lambda a, b: a + b, [hist1[j] for j in range(cols)])

    @pl.loop(1, rows)
    def _(k):
        pltpu.make_async_remote_copy(
            src_ref=hist2.at[r], dst_ref=hist2.at[r], send_sem=h2_send, recv_sem=h2_recv,
            device_id=(lax.rem(r + k, rows), c), device_id_type=MESH).start()

    hist2_rest = hist2.at[pl.ds(0, rows - 1)]
    pltpu.make_async_copy(hist2_rest, hist2_rest, h2_recv).wait()
    total = functools.reduce(lambda a, b: a + b, [hist2[j] for j in range(rows)])
    rate_ref[...] = total[0:groups] / jnp.maximum(total[groups : 2 * groups], 1.0)

    keep.wait()
    pltpu.make_async_copy(smalls_rest, smalls_rest, small_send).wait()
    pltpu.make_async_copy(hist1_rest, hist1_rest, h1_send).wait()
    pltpu.make_async_copy(hist2_rest, hist2_rest, h2_send).wait()
    others = tables_ref.at[pl.ds(0, rows * chips - 1)]
    pltpu.make_async_copy(others, others, table_send).wait()
    passed = tables_ref.at[pl.ds(0, rows * chips)]
    pltpu.make_async_copy(passed, passed, pass_send).wait()
    pltpu.make_async_copy(passed, passed, pass_recv).wait()


def join_kernel(tables_ref, smalls_ref, pkey_ref, ppart_ref, place_ref, rate_ref, joined_ref, place_out, rate_out):
    owner = pl.program_id(0)
    rows, _, depth, width = tables_ref.shape
    probe_tiles, tile_rows = pkey_ref.shape[3], pkey_ref.shape[4]
    table = tables_ref[:, owner].reshape(rows * depth, width)
    high = table.astype(jnp.bfloat16)
    low = (table - high.astype(jnp.float32)).astype(jnp.bfloat16)
    both = jnp.concatenate([high, low], axis=1)
    keys = pkey_ref[0, 0, 0]
    code = jnp.where(keys >= 0, ppart_ref[0, 0, 0] * KEY_RANGE + keys, -1).astype(jnp.float32)
    code = code.T
    wanted = [smalls_ref[s, owner, 2:3, :] for s in range(rows)]
    hot = []
    for q in range(probe_tiles):
        wide = jnp.broadcast_to(code[:, q : q + 1], (tile_rows, depth))
        hot.append(jnp.concatenate(
            [jnp.where(wide == want, 1.0, 0.0).astype(jnp.bfloat16) for want in wanted], axis=1))
    out = jnp.dot(jnp.concatenate(hot, axis=0), both, preferred_element_type=jnp.float32)
    joined_ref[0, 0, 0] = (out[:, :width] + out[:, width:]).reshape(probe_tiles, tile_rows, width)
    place_out[...] = place_ref[owner].reshape(place_out.shape)
    rate_out[...] = rate_ref[...]


def local(build_key, build_part, build_payload, probe_key, probe_part):
    rows, cols = lax.axis_size("row"), lax.axis_size("col")
    n = rows * cols
    local_tiles = build_key.shape[1]
    width = build_payload.shape[-1]
    owners, probe_tiles, tile_rows = probe_key.shape[2:]
    depth = local_tiles * KEY_RANGE
    groups = PARTS_SIZE // LANES
    vmem = pl.BlockSpec(memory_space=pltpu.VMEM)
    dma = pltpu.SemaphoreType.DMA
    f32 = jnp.float32
    tables, smalls, places, rate = pl.pallas_call(
        functools.partial(gather_kernel, rows, cols, local_tiles),
        out_shape=(
            jax.ShapeDtypeStruct((n, depth, width), f32),
            jax.ShapeDtypeStruct((n, 8, depth), f32),
            jax.ShapeDtypeStruct((owners, probe_tiles, tile_rows), f32),
            jax.ShapeDtypeStruct((groups, LANES), f32),
        ),
        in_specs=[pl.BlockSpec(memory_space=pltpu.HBM)] * 5,
        out_specs=(vmem, vmem, vmem, vmem),
        scratch_shapes=[
            pltpu.VMEM(build_key.shape, build_key.dtype),
            pltpu.SMEM(build_part.shape, build_part.dtype),
            pltpu.VMEM(build_payload.shape, f32),
            pltpu.VMEM(probe_key.shape, probe_key.dtype),
            pltpu.VMEM(probe_part.shape, probe_part.dtype),
            pltpu.VMEM((depth, width), f32),
            pltpu.VMEM((cols, 2 * groups, LANES), f32),
            pltpu.VMEM((rows, 2 * groups, LANES), f32),
            dma((5,)),
            dma, dma, dma, dma((rows * (cols // 2),)), dma, dma,
            dma, dma, dma, dma, dma,
        ],
        compiler_params=pltpu.CompilerParams(
            collective_id=0, has_side_effects=True, vmem_limit_bytes=40 * 1024 * 1024
        ),
    )(build_key, build_part, build_payload, probe_key, probe_part)
    tables = tables.reshape(rows, cols, depth, width)
    smalls = smalls.reshape(rows, cols, 8, depth)
    joined, placed, rate = pl.pallas_call(
        join_kernel,
        grid=(owners,),
        out_shape=(
            jax.ShapeDtypeStruct((1, 1, owners, probe_tiles, tile_rows, width), f32),
            jax.ShapeDtypeStruct((1, 1, owners, probe_tiles, tile_rows), f32),
            jax.ShapeDtypeStruct((groups, LANES), f32),
        ),
        in_specs=[
            vmem,
            vmem,
            pl.BlockSpec((1, 1, 1, probe_tiles, tile_rows), lambda i: (0, 0, i, 0, 0)),
            pl.BlockSpec((1, 1, 1, probe_tiles, tile_rows), lambda i: (0, 0, i, 0, 0)),
            vmem,
            vmem,
        ],
        out_specs=(
            pl.BlockSpec((1, 1, 1, probe_tiles, tile_rows, width), lambda i: (0, 0, i, 0, 0, 0)),
            pl.BlockSpec((1, 1, 1, probe_tiles, tile_rows), lambda i: (0, 0, i, 0, 0)),
            pl.BlockSpec((groups, LANES), lambda i: (0, 0)),
        ),
        compiler_params=pltpu.CompilerParams(vmem_limit_bytes=24 * 1024 * 1024),
    )(tables, smalls, probe_key, probe_part, places, rate)
    return joined, placed, rate.reshape(PARTS_SIZE)


def solution(mesh):
    return jax.shard_map(
        local,
        mesh=mesh,
        in_specs=(
            P("col", "row", None),
            P("col", "row"),
            P("col", "row", None, None),
            P("row", "col", None, None, None),
            P("row", "col", None, None, None),
        ),
        out_specs=(P("row", "col", None, None, None, None), P("row", "col", None, None, None), P()),
        check_vma=False,
    )
```
